32 devices in a mesh: gx: 2 (over x), gy: 4 (over z), gz: 4 (over y, core).
Axes of the slice: x: 2, y: 2, z: 4, core: 2. Of those that a mesh axis runs over, the one named last changes fastest.
Arguments:
- pair_list: int32 [1024, 2], P(('gx', 'gy', 'gz')), may hold values from 0 to 63, all different within a row; in each aligned block of 32 rows (0 to 31, 32 to 63, ...) at most 2 rows name the same one
- rank_bucket: int32 [1024], P(('gx', 'gy', 'gz')), may hold values from 0 to 2
- amplitudes: bfloat16 [1024, 36864], P(('gx', 'gy', 'gz')), may hold values from -0.4375 to 0.4375
- intersects: bfloat16 [1024, 36864], P(('gx', 'gy', 'gz')), may hold values from -0.4375 to 0.4375
- integrals: bfloat16 [1024, 36864], P(('gx', 'gy', 'gz')), may hold values from -6 to 6
- exchange_blocks: bfloat16 [64, 36864], P(('gx', 'gy')), may hold values from -0.4375 to 0.4375
Outputs:
- residuals: bfloat16 [1024, 36864], P(('gx', 'gy', 'gz'))
The draws below stay inside these ranges and needn't reach their ends.
Inputs may be any that keep to these rules, and one draw needn't show every extreme that they name: `pair_list`: each row names two different occupied orbitals; within the rows of one device no orbital is named more than 2 times, a bound that some block reaches on some devices. `rank_bucket`: bucket b keeps the leading (b + 1) * 64 PNOs.
All inputs are finite; a program needn't handle non-finite values.
Results may differ from the reference program's by a relative error of at most 0.013.
Values may be sent and summed in bfloat16 or wider, within the bound.
A program may use at most 128 MiB of HBM per device.

```python
import math
import jax
import jax.numpy as jnp
import numpy as np
from jax import lax

RSTEP = 64
R = 192
NOCC = 64
MOST = 2
PAIR_DEV = 32
NPAIRS = 1024


def touch_ends(values, stream_key, least, top_value):
    place = [jax.random.randint(jax.random.fold_in(stream_key, axis), (), 0, length) for axis, length in enumerate(values.shape)]
    main_axis = values.shape.index(max(values.shape))
    neighbour = place[:main_axis] + [(place[main_axis] + 1) % values.shape[main_axis]] + place[main_axis + 1:]
    return values.at[tuple(place)].set(least).at[tuple(neighbour)].set(top_value)


def levels(key, shape, split, least, high):
    def one(dim, parts):
        heights = jax.random.uniform(jax.random.fold_in(jax.random.fold_in(key, 6), dim), (parts,), jnp.float32, least / len(split), high / len(split))
        return jnp.repeat(jnp.exp(heights), shape[dim] // parts).reshape((-1,) + (1,) * (len(shape) - dim - 1))

    gain = one(*split[0])
    for cut in split[1:]:
        gain = gain * one(*cut)
    return gain


def deal_out(rng, own, number, rows, amount, top, bound, lean):
    order = jax.random.permutation(rng, amount)
    heavy_load, ordinary = load_shares(amount, rows * top, bound, lean, True), load_shares(amount, rows * top, bound, lean, False)
    places = jnp.arange(amount)

    def named(tallies, turn):
        used = int((tallies > 0).sum())
        fixed = max(1, used // 4)
        passed = fixed + (places - fixed + turn * (used - fixed)) % max(1, amount - fixed)
        return jnp.zeros((amount,), jnp.int32).at[order[jnp.where(places < fixed, places, passed)]].set(jnp.asarray(tallies, jnp.int32))

    tallies = jnp.where(number % 4 == 0, named(heavy_load, number // 4), named(ordinary, number - number // 4 - 1))
    mixed = jax.random.permutation(jax.random.fold_in(own, 3), amount)
    giver, receiver = mixed[0:amount // 2 * 2:2], mixed[1:amount // 2 * 2:2]
    slack = jnp.minimum(tallies[giver] - 1, bound - tallies[receiver]) // 2
    slack = jnp.where((giver == order[0]) | (receiver == order[0]) | (tallies[receiver] == 0), 0, jnp.maximum(slack, 0))
    passed = jax.random.randint(jax.random.fold_in(own, 4), (amount // 2,), 0, 1 << 20) % (slack + 1)
    tallies = tallies.at[giver].add(-passed).at[receiver].add(passed)
    items = jnp.searchsorted(jnp.cumsum(tallies), jnp.arange(rows * top), side="right").astype(jnp.int32)
    listing = items.reshape(top, rows).T
    listing = listing[jax.random.permutation(jax.random.fold_in(own, 1), rows)]
    turn = jax.random.randint(jax.random.fold_in(own, 2), (rows, 1), 0, top)
    return jnp.take_along_axis(listing, (jnp.arange(top)[None, :] + turn) % top, axis=1)


def load_shares(count, total, bound, slope, full):
    portions = [(1 << 20) // math.isqrt(standing ** slope) + 1 for standing in range(1, count + 1)]
    largest = bound if full else min(bound, max(-(-total // count), total * portions[0] // sum(portions)))
    least = 1 if total - largest >= count - 1 else 0
    holding, surplus = [largest] + [least] * (count - 1), total - largest - least * (count - 1)
    while surplus > 0:
        movable = [i for i in range(1, count) if holding[i] < largest] or [i for i in range(1, count) if holding[i] < bound]
        pool, remaining = sum([portions[i] for i in movable]), surplus
        for i in movable:
            extra = min(bound - holding[i], max(1, remaining * portions[i] // pool), surplus)
            holding[i] = holding[i] + extra
            surplus = surplus - extra
    return np.array(holding)


def scatter_about(rng, shape, scale, limit, cuts=(), kind=jnp.bfloat16):
    values = scale * jax.random.normal(rng, shape, jnp.float32)
    if cuts:
        values = values * levels(rng, shape, cuts, -0.22, 0.18)
    return jnp.clip(values, -limit, limit).astype(kind)


def setup_inputs(seed: int = 0) -> dict:
    keys = jax.random.split(jax.random.key(seed), 7)
    pair_list_keys = jax.random.split(jax.random.fold_in(keys[0], 1), NPAIRS // PAIR_DEV)
    pair_list_turns = jax.random.permutation(jax.random.fold_in(keys[0], 3), NPAIRS // PAIR_DEV)
    pair_list = jax.vmap(lambda own, number: deal_out(jax.random.fold_in(keys[0], 2), own, number, PAIR_DEV, NOCC, 2, MOST, 2))(pair_list_keys, pair_list_turns).reshape((NPAIRS, 2))
    rank_bucket = touch_ends(jax.random.randint(keys[1], (NPAIRS,), 0, 3), jax.random.fold_in(keys[1], 1), 0, 2).astype(jnp.int32)
    amplitudes = scatter_about(keys[2], (NPAIRS, R * R), R ** -0.5, 0.4375, ((0, 32),))
    intersects = scatter_about(keys[3], (NPAIRS, R * R), R ** -0.5, 0.4375, ((0, 32),))
    integrals = scatter_about(keys[4], (NPAIRS, R * R), 1.0, 6.0, ((0, 32),))
    exchange_blocks = scatter_about(keys[5], (NOCC, R * R), R ** -0.5, 0.4375, ((0, 8),))
    return {"pair_list": pair_list, "rank_bucket": rank_bucket, "amplitudes": amplitudes, "intersects": intersects, "integrals": integrals, "exchange_blocks": exchange_blocks}


def rounded(value):
    return lax.optimization_barrier(value.astype(jnp.bfloat16)).astype(jnp.float32)


def rank_mask(bucket):
    rank_size = (bucket + 1) * RSTEP
    row_index = jnp.arange(R, dtype=jnp.int32)
    return (row_index[None, :, None] < rank_size[:, None, None]) & (row_index[None, None, :] < rank_size[:, None, None])


def project_block(inputs):
    bucket, amplitude, intersect = inputs
    inside = rank_mask(bucket)
    masked = jnp.where(inside, amplitude, jnp.zeros_like(amplitude))
    half_projected = rounded(jnp.einsum('pab,pbc->pac', intersect.astype(jnp.float32), masked.astype(jnp.float32)))
    return jnp.einsum('pab,pcb->pac', half_projected, intersect.astype(jnp.float32)).astype(jnp.bfloat16)


def reference(pair_list, rank_bucket, amplitudes, intersects, integrals, exchange_blocks):
    blocks = NPAIRS // PAIR_DEV
    block_shape = (blocks, PAIR_DEV, R, R)
    exchange_square = exchange_blocks.reshape(NOCC, R, R)
    bucket_blocks = rank_bucket.reshape(blocks, PAIR_DEV)
    list_blocks = pair_list.reshape(blocks, PAIR_DEV, 2)
    amplitude_blocks = amplitudes.reshape(block_shape)
    intersect_blocks = intersects.reshape(block_shape)
    integral_blocks = integrals.reshape(block_shape)
    projected = lax.map(project_block, (bucket_blocks, amplitude_blocks, intersect_blocks))

    def accumulate(domain, inputs):
        ends_block, projected_block = inputs
        as_float = projected_block.astype(jnp.float32)
        domain = domain + jax.ops.segment_sum(as_float, ends_block[:, 0], num_segments=NOCC)
        domain = domain + jax.ops.segment_sum(as_float, ends_block[:, 1], num_segments=NOCC)
        return domain, None

    domain, unused = lax.scan(accumulate, jnp.zeros((NOCC, R, R), jnp.float32), (list_blocks, projected))
    coupled = rounded(jnp.einsum('oab,obc->oac', rounded(domain), exchange_square.astype(jnp.float32)))

    def finish(inputs):
        ends_block, bucket, projected_block, intersect, integral, amplitude = inputs
        inside = rank_mask(bucket)
        masked = jnp.where(inside, amplitude, jnp.zeros_like(amplitude))
        combined = jnp.zeros((PAIR_DEV, R, R), jnp.float32)
        for which_end in range(2):
            orbital = ends_block[:, which_end]
            own_term = rounded(jnp.einsum('pab,pbc->pac', projected_block.astype(jnp.float32), exchange_square[orbital].astype(jnp.float32)))
            answer = rounded(coupled[orbital] - own_term)
            combined = combined + answer
        combined = rounded(combined)
        half_back = rounded(jnp.einsum('pba,pbc->pac', intersect.astype(jnp.float32), combined))
        back_projected = jnp.einsum('pab,pbc->pac', half_back, intersect.astype(jnp.float32))
        local_term = jnp.einsum('pab,pbc->pac', masked.astype(jnp.float32), integral.astype(jnp.float32))
        residual_sum = integral.astype(jnp.float32) + local_term + back_projected
        return jnp.where(inside, residual_sum, jnp.zeros_like(residual_sum)).astype(jnp.bfloat16)

    result = lax.map(finish, (list_blocks, bucket_blocks, projected, intersect_blocks, integral_blocks, amplitude_blocks))
    return result.reshape(NPAIRS, R * R)
```

```python
import functools

import jax
import jax.numpy as jnp
import numpy as np
from jax import lax
from jax.experimental import pallas as pl
from jax.experimental.pallas import tpu as pltpu
from jax.sharding import PartitionSpec as P

RSTEP = 64
R = 192
LANES = 128
PIECES = 2
AXES = ("gx", "gy", "gz")
MESH = pl.DeviceIdType.MESH
BF = jnp.bfloat16
F32 = jnp.float32


def bits_of(mesh_shape):
    found, stride = {}, 1
    for axis in reversed(AXES):
        size = mesh_shape[axis]
        found[axis] = [(axis, 1 << b, stride << b) for b in range(size.bit_length() - 1)]
        stride *= size
    return found


def orders_of(mesh_shape):
    b = bits_of(mesh_shape)
    first, rest = b["gz"][:1], b["gz"][1:]
    return (first + rest + b["gx"] + b["gy"], first + b["gx"] + rest + b["gy"])


def dot(a, b, dims=((1,), (0,))):
    return lax.dot_general(a, b, (dims, ((), ())), preferred_element_type=F32)


def kernel(
    orders, rank_ref, named_ref, where_ref, amp_ref, int_ref, itg_ref, xown_ref, out_ref,
    proj, acc, land, cbuf, xbuf, own, loc, turned, send_sem, recv_sem,
):
    pairs = amp_ref.shape[0]
    stages = len(orders[0])
    units = 1 << stages
    rows = R // PIECES

    def partner(bit):
        axis, stride, _ = bit
        c = lax.axis_index(axis)
        return {axis: c + stride * (1 - 2 * ((c // stride) % 2))}

    order_of = [h % 2 for h in range(PIECES)]
    bit_of = lambda h, s: orders[order_of[h]][s]
    half = lambda s: units >> (s + 1)

    barrier = pltpu.get_barrier_semaphore()
    for bit in orders[0]:
        pl.semaphore_signal(barrier, inc=1, device_id=partner(bit), device_id_type=MESH)
    pl.semaphore_wait(barrier, stages)

    def remote(kind, src, dst, h, s):
        return pltpu.make_async_remote_copy(
            src_ref=src, dst_ref=dst, send_sem=send_sem.at[kind, h, s], recv_sem=recv_sem.at[kind, h, s],
            device_id=partner(bit_of(h, s)), device_id_type=MESH,
        )

    def reduce_copy(h, s):
        n = half(s)
        return remote(0, acc.at[h, pl.ds(n, n)], land.at[h, pl.ds(n, n)], h, s)

    def gather_copy(kind, buf, h, s):
        n = half(s)
        return remote(kind, buf.at[h, pl.ds(0, n)], buf.at[h, pl.ds(n, n)], h, s)

    def pack(ref, h, j, a, b):
        ref[h, j, 0] = a[:, :LANES]
        ref[h, j, 1] = b[:, :LANES]
        ref[h, j, 2] = jnp.concatenate([a[:, LANES:], b[:, LANES:]], axis=1)

    for h in range(PIECES):
        span = pl.ds(h * rows, rows)
        pack(xbuf, h, 0, xown_ref[0, span], xown_ref[1, span])
    for h in range(PIECES):
        gather_copy(2, xbuf, h, stages - 1).start()

    def x_step(s):
        for h in range(PIECES):
            gather_copy(2, xbuf, h, s).wait_recv()
            if s:
                gather_copy(2, xbuf, h, s - 1).start()

    row = lax.broadcasted_iota(jnp.int32, (R, R), 0)
    col = lax.broadcasted_iota(jnp.int32, (R, R), 1)
    reach = jnp.maximum(row, col)

    def masked(p):
        size = (rank_ref[p] + 1) * RSTEP
        return jnp.where(reach < size, amp_ref[p].astype(F32), 0.0).astype(BF)

    def project(p, carry):
        side = int_ref[p]
        h1 = dot(side, masked(p)).astype(BF)
        proj[p] = dot(h1, side, ((1,), (1,))).astype(BF)
        return carry

    proj[pairs] = jnp.zeros((R, R), BF)
    cut = [pairs * i // stages for i in range(stages + 1)]
    waits = list(range(stages - 1, 0, -1))
    for i in range(stages):
        lax.fori_loop(cut[i], cut[i + 1], project, 0, unroll=2)
        if i < len(waits) - 1:
            x_step(waits[i])

    def build(h, j, carry):
        span = pl.ds(h * rows, rows)
        base = (order_of[h] * units + j) * 4
        a = proj[named_ref[base], span] + proj[named_ref[base + 1], span]
        b = proj[named_ref[base + 2], span] + proj[named_ref[base + 3], span]
        pack(acc, h, j, a, b)
        return carry

    for h in range(PIECES):
        lax.fori_loop(units // 2, units, functools.partial(build, h), 0)
        reduce_copy(h, 0).start()
    x_step(1)
    for h in range(PIECES):
        lax.fori_loop(0, units // 2, functools.partial(build, h), 0)

    def local(p, carry):
        block = itg_ref[p]
        loc[p] = dot(masked(p), block) + block.astype(F32)
        turned[p] = int_ref[p].T
        return carry

    def fetch(buf, p, e):
        base = (p * 2 + e) * 3
        odd = where_ref[base + 2]
        parts = []
        for h in range(PIECES):
            at = where_ref[base + order_of[h]]
            tail = buf[h, at, 2]
            tail = jnp.where(odd == 1, tail[:, LANES // 2 :], tail[:, : LANES // 2])
            parts.append(jnp.concatenate([buf[h, at, odd], tail], axis=1))
        return jnp.concatenate(parts, axis=0)

    def own_part(p, carry):
        both = fetch(xbuf, p, 0) + fetch(xbuf, p, 1)
        own[p] = dot(proj[p], both).astype(BF)
        return carry

    def add(h, n, j, carry):
        acc[h, j] = acc[h, j] + land[h, n + j]
        return carry

    def reduce_step(s):
        n = half(s)
        for h in range(PIECES):
            reduce_copy(h, s).wait_recv()
            lax.fori_loop(n // 2, n, functools.partial(add, h, n), 0)
            if s + 1 < stages:
                reduce_copy(h, s + 1).start()
        for h in range(PIECES):
            lax.fori_loop(0, n // 2, functools.partial(add, h, n), 0)

    quarter = pairs // 4
    reduce_step(0)
    lax.fori_loop(0, pairs, local, 0, unroll=2)
    reduce_step(1)
    x_step(0)
    lax.fori_loop(0, 2 * quarter, own_part, 0, unroll=2)
    reduce_step(2)
    lax.fori_loop(2 * quarter, 3 * quarter, own_part, 0, unroll=2)
    for s in range(3, stages):
        reduce_step(s)

    for h in range(PIECES):
        left = [acc[h, 0, t] for t in range(2)]
        tail = acc[h, 0, 2]
        done = []
        for t in range(2):
            block = jnp.concatenate([left[t], tail[:, t * (LANES // 2) : (t + 1) * (LANES // 2)]], axis=1)
            done.append(dot(block, xown_ref[t]).astype(BF))
        pack(cbuf, h, 0, *done)
        gather_copy(1, cbuf, h, stages - 1).start()
    lax.fori_loop(3 * quarter, pairs, own_part, 0, unroll=2)
    for s in range(stages - 1, -1, -1):
        for h in range(PIECES):
            gather_copy(1, cbuf, h, s).wait_recv()
            if s:
                gather_copy(1, cbuf, h, s - 1).start()

    def finish(p, carry):
        total = fetch(cbuf, p, 0).astype(F32) + fetch(cbuf, p, 1).astype(F32) - own[p].astype(F32)
        half_back = dot(turned[p], total.astype(BF)).astype(BF)
        result = loc[p] + dot(half_back, int_ref[p])
        size = (rank_ref[p] + 1) * RSTEP
        out_ref[p] = jnp.where(reach < size, result, 0.0).astype(BF)
        return carry

    lax.fori_loop(0, pairs, finish, 0, unroll=2)

    for h in range(PIECES):
        for s in range(stages):
            reduce_copy(h, s).wait_send()
            gather_copy(1, cbuf, h, s).wait_send()
            gather_copy(2, xbuf, h, s).wait_send()


def fused(orders, pair_list, rank_bucket, amplitudes, intersects, integrals, exchange_blocks):
    pairs = amplitudes.shape[0]
    stages = len(orders[0])
    units = 1 << stages
    me = jnp.int32(0)
    for axis in AXES:
        me = me * lax.axis_size(axis) + lax.axis_index(axis)

    named, where = [], []
    unit_of_end = pair_list // 2
    for order in orders:
        at = np.arange(units)
        relative = sum(((at >> (stages - 1 - s)) & 1) * order[s][2] for s in range(stages))
        orbital = 2 * (jnp.asarray(relative, jnp.int32) ^ me)[:, None] + jnp.arange(2, dtype=jnp.int32)[None]
        hit = jnp.any(pair_list[None, None] == orbital[:, :, None, None], axis=3)
        spot = jnp.arange(pairs, dtype=jnp.int32)
        first = jnp.min(jnp.where(hit, spot, pairs), axis=2)
        last = jnp.max(jnp.where(hit, spot, -1), axis=2)
        last = jnp.where(last > first, last, pairs)
        named.append(jnp.stack([first, last], axis=2).reshape(-1))
        apart = unit_of_end ^ me
        where.append(sum(((apart // order[s][2]) % 2) << (stages - 1 - s) for s in range(stages)))
    where.append(pair_list % 2)
    named = jnp.concatenate(named)
    where = jnp.stack(where, axis=2).reshape(-1)

    square = lambda a: a.reshape(a.shape[0], R, R)
    mine = lax.dynamic_slice_in_dim(exchange_blocks, lax.axis_index("gz") * 2, 2, 0)
    rows = R // PIECES
    whole = (PIECES, units, 3, rows, LANES)
    smem = pl.BlockSpec(memory_space=pltpu.SMEM)
    vmem = pl.BlockSpec(memory_space=pltpu.VMEM)
    result = pl.pallas_call(
        functools.partial(kernel, orders),
        out_shape=jax.ShapeDtypeStruct((pairs, R, R), BF),
        in_specs=[smem] * 3 + [vmem] * 4,
        out_specs=vmem,
        scratch_shapes=[
            pltpu.VMEM((pairs + 1, R, R), BF),
            pltpu.VMEM(whole, BF),
            pltpu.VMEM(whole, BF),
            pltpu.VMEM(whole, BF),
            pltpu.VMEM(whole, BF),
            pltpu.VMEM((pairs, R, R), BF),
            pltpu.VMEM((pairs, R, R), F32),
            pltpu.VMEM((pairs, R, R), BF),
            pltpu.SemaphoreType.DMA((3, PIECES, stages)),
            pltpu.SemaphoreType.DMA((3, PIECES, stages)),
        ],
        compiler_params=pltpu.CompilerParams(
            collective_id=0, has_side_effects=True, vmem_limit_bytes=60 * 1024 * 1024
        ),
    )(rank_bucket, named, where, square(amplitudes), square(intersects), square(integrals), square(mine))
    return result.reshape(pairs, R * R)


def plain(pair_list, rank_bucket, amplitudes, intersects, integrals, exchange_blocks):
    pair_rows, owned_rows = amplitudes.shape[0], exchange_blocks.shape[0]
    square = lambda a: a.reshape(a.shape[0], R, R)
    amplitudes, intersects, integrals = map(square, (amplitudes, intersects, integrals))
    exchange_blocks = square(exchange_blocks)
    occupied = owned_rows * lax.axis_size("gx") * lax.axis_size("gy")
    reach = jnp.maximum(lax.broadcasted_iota(jnp.int32, (R, R), 0), lax.broadcasted_iota(jnp.int32, (R, R), 1))
    inside = reach[None] < ((rank_bucket + 1) * RSTEP)[:, None, None]
    ein = functools.partial(jnp.einsum, preferred_element_type=F32)
    masked = jnp.where(inside, amplitudes, jnp.zeros_like(amplitudes))
    half_projected = ein("pab,pbc->pac", intersects, masked).astype(BF)
    projected = ein("pab,pcb->pac", half_projected, intersects).astype(BF)
    local_term = ein("pab,pbc->pac", masked, integrals)
    counts = jnp.sum(
        (pair_list[None] == lax.broadcasted_iota(jnp.int32, (occupied, 1, 1), 0)).astype(jnp.int32), axis=2
    ).astype(BF)
    share = jnp.dot(counts, projected.reshape(pair_rows, R * R), preferred_element_type=F32)
    share = lax.psum_scatter(share, ("gx", "gy"), scatter_dimension=0, tiled=True)
    domain = lax.psum(share.reshape(owned_rows, R, R), "gz")
    coupled = ein("oab,obc->oac", domain.astype(BF), exchange_blocks).astype(BF)
    every_coupled = lax.all_gather(coupled, ("gx", "gy"), axis=0, tiled=True)
    every_block = lax.all_gather(exchange_blocks, ("gx", "gy"), axis=0, tiled=True)
    own_term = ein("pab,pebc->peac", projected, every_block[pair_list]).astype(BF)
    answers = (every_coupled[pair_list].astype(F32) - own_term.astype(F32)).astype(BF)
    combined = (answers[:, 0].astype(F32) + answers[:, 1].astype(F32)).astype(BF)
    half_back = ein("pba,pbc->pac", intersects, combined).astype(BF)
    total = integrals.astype(F32) + local_term + ein("pab,pbc->pac", half_back, intersects)
    return jnp.where(inside, total, jnp.zeros_like(total)).astype(BF).reshape(pair_rows, R * R)


def solution(mesh):
    shape = dict(mesh.shape)
    split = P(AXES, None)
    powers = all(shape[a] & (shape[a] - 1) == 0 for a in AXES) and shape["gz"] > 1

    def body(*args):
        if powers and args[5].shape[0] == 2 * shape["gz"]:
            return fused(orders_of(shape), *args)
        return plain(*args)

    return jax.shard_map(
        body, mesh=mesh, in_specs=(split, P(AXES), split, split, split, P(("gx", "gy"), None)),
        out_specs=split, check_vma=False,
    )
```

```python
import functools

import jax
import jax.numpy as jnp
import numpy as np
from jax import lax
from jax.experimental import pallas as pl
from jax.experimental.pallas import tpu as pltpu
from jax.sharding import PartitionSpec as P

RSTEP = 64
R = 192
LANES = 128
PIECES = 4
LAG = 1
X3, X2, X1, X0 = 1, 2, 4, 7
AXES = ("gx", "gy", "gz")
MESH = pl.DeviceIdType.MESH
BF = jnp.bfloat16
F32 = jnp.float32


def bits_of(mesh_shape):
    found, stride = {}, 1
    for axis in reversed(AXES):
        size = mesh_shape[axis]
        found[axis] = [(axis, 1 << b, stride << b) for b in range(size.bit_length() - 1)]
        stride *= size
    return found


def orders_of(mesh_shape):
    b = bits_of(mesh_shape)
    first, rest = b["gz"][:1], b["gz"][1:]
    return (first + rest + b["gx"] + b["gy"], first + b["gx"] + rest + b["gy"])


def dot(a, b, dims=((1,), (0,))):
    return lax.dot_general(a, b, (dims, ((), ())), preferred_element_type=F32)


def kernel(
    orders, rank_ref, named_ref, where_ref, amp_raw, int_raw, itg_raw, xown_raw, out_ref,
    amp_ref, int_ref, itg_ref, xown_ref, proj, acc, land, cbuf, xbuf, own, loc, turned, send_sem, recv_sem,
):
    pairs = amp_raw.shape[0]
    stages = len(orders[0])
    units = 1 << stages
    rows = R // PIECES

    def partner(bit):
        axis, stride, _ = bit
        c = lax.axis_index(axis)
        return {axis: c + stride * (1 - 2 * ((c // stride) % 2))}

    order_of = [h % 2 for h in range(PIECES)]
    bit_of = lambda h, s: orders[order_of[h]][s]
    half = lambda s: units >> (s + 1)

    barrier = pltpu.get_barrier_semaphore()
    for bit in orders[0]:
        pl.semaphore_signal(barrier, inc=1, device_id=partner(bit), device_id_type=MESH)
    pl.semaphore_wait(barrier, stages)

    def remote(kind, src, dst, h, s):
        return pltpu.make_async_remote_copy(
            src_ref=src, dst_ref=dst, send_sem=send_sem.at[kind, h, s], recv_sem=recv_sem.at[kind, h, s],
            device_id=partner(bit_of(h, s)), device_id_type=MESH,
        )

    def reduce_copy(h, s):
        n = half(s)
        return remote(0, acc.at[h, pl.ds(n, n)], land.at[h, pl.ds(n, n)], h, s)

    def gather_copy(kind, buf, h, s):
        n = half(s)
        return remote(kind, buf.at[h, pl.ds(0, n)], buf.at[h, pl.ds(n, n)], h, s)

    def pack(ref, h, j, a, b):
        ref[h, j, 0] = a[:, :LANES]
        ref[h, j, 1] = b[:, :LANES]
        ref[h, j, 2] = jnp.concatenate([a[:, LANES:], b[:, LANES:]], axis=1)

    row = lax.broadcasted_iota(jnp.int32, (R, R), 0)
    col = lax.broadcasted_iota(jnp.int32, (R, R), 1)
    natural = jnp.where(row < R // 2, 2 * row, 2 * row - (R - 1))
    reach = jnp.maximum(natural, col)
    sort = (natural == col).astype(F32).astype(BF)

    unsort = (lax.broadcasted_iota(jnp.int32, (R, R), 0) == jnp.where(col < R // 2, 2 * col, 2 * col - (R - 1))).astype(F32).astype(BF)

    for t in range(2):
        xown_ref[t] = dot(dot(sort, xown_raw[t]).astype(BF), sort, ((1,), (1,))).astype(BF)
    for h in range(PIECES):
        span = pl.ds(h * rows, rows)
        pack(xbuf, h, 0, xown_ref[0, span], xown_ref[1, span])
    for h in range(PIECES):
        gather_copy(2, xbuf, h, stages - 1).start()

    def x_step(s):
        for h in range(PIECES):
            gather_copy(2, xbuf, h, s).wait_recv()
            if s:
                gather_copy(2, xbuf, h, s - 1).start()

    def relayout(raw, ref):
        def some(c, carry):
            at = pl.multiple_of(c * 16 * 2 * R, LANES)
            top = pl.multiple_of(c * 16, 16)
            low = pl.multiple_of(R // 2 + c * 16, 16)
            for g in range(0, pairs, 16):
                value = raw[g : g + 16, pl.ds(at, 16 * 2 * R)].reshape(16, 16, 2 * R)
                ref[pl.ds(g, 16), pl.ds(top, 16), :] = value[:, :, :R]
                ref[pl.ds(g, 16), pl.ds(low, 16), :] = value[:, :, R:]
            return carry

        lax.fori_loop(0, R // 32, some, 0)

    def masked(p):
        size = (rank_ref[p] + 1) * RSTEP
        return jnp.where(reach < size, amp_ref[p].astype(F32), 0.0).astype(BF)

    def project(p, carry):
        side = int_ref[p]
        middle = dot(unsort, masked(p)).astype(BF)
        h1 = dot(side, middle).astype(BF)
        proj[p] = dot(h1, side, ((1,), (1,))).astype(BF)
        return carry

    proj[pairs] = jnp.zeros((R, R), BF)
    relayout(amp_raw, amp_ref)
    relayout(int_raw, int_ref)
    lax.fori_loop(0, pairs // 2, project, 0, unroll=2)
    x_step(stages - 1)
    lax.fori_loop(pairs // 2, pairs, project, 0, unroll=2)

    def build(h, j, carry):
        span = pl.ds(h * rows, rows)
        base = (order_of[h] * units + j) * 4
        a = proj[named_ref[base], span] + proj[named_ref[base + 1], span]
        b = proj[named_ref[base + 2], span] + proj[named_ref[base + 3], span]
        pack(acc, h, j, a, b)
        return carry

    for h in range(PIECES):
        lax.fori_loop(units // 2, units, functools.partial(build, h), 0)
        reduce_copy(h, 0).start()
    for h in range(PIECES):
        lax.fori_loop(0, units // 2, functools.partial(build, h), 0)

    def local(p, carry):
        block = itg_ref[p]
        middle = dot(unsort, block).astype(BF)
        loc[p] = dot(masked(p), middle) + block.astype(F32)
        turned[p] = dot(sort, int_ref[p], ((1,), (1,))).astype(BF)
        return carry

    def fetch(buf, p, e):
        base = (p * 2 + e) * 3
        odd = where_ref[base + 2]
        parts = []
        for h in range(PIECES):
            at = where_ref[base + order_of[h]]
            tail = buf[h, at, 2]
            tail = jnp.where(odd == 1, tail[:, LANES // 2 :], tail[:, : LANES // 2])
            parts.append(jnp.concatenate([buf[h, at, odd], tail], axis=1))
        return jnp.concatenate(parts, axis=0)

    def own_part(p, carry):
        both = fetch(xbuf, p, 0) + fetch(xbuf, p, 1)
        own[p] = dot(proj[p], both).astype(BF)
        return carry

    def add(h, n, j, carry):
        acc[h, j] = acc[h, j] + land[h, n + j]
        return carry

    def couple(h):
        tail = acc[h, 0, 2]
        done = []
        for t in range(2):
            block = jnp.concatenate([acc[h, 0, t], tail[:, t * (LANES // 2) : (t + 1) * (LANES // 2)]], axis=1)
            done.append(dot(block, xown_ref[t]).astype(BF))
        pack(cbuf, h, 0, *done)
        gather_copy(1, cbuf, h, stages - 1).start()

    def advance(h, step):
        if step >= stages:
            s = 2 * stages - 1 - step
            gather_copy(1, cbuf, h, s).wait_recv()
            if s:
                gather_copy(1, cbuf, h, s - 1).start()
            return
        n = half(step)
        reduce_copy(h, step).wait_recv()
        lax.fori_loop(n // 2, n, functools.partial(add, h, n), 0)
        if step + 1 < stages:
            reduce_copy(h, step + 1).start()
        lax.fori_loop(0, n // 2, functools.partial(add, h, n), 0)
        if step + 1 == stages:
            couple(h)

    groups = PIECES // 2
    last = groups - 1
    after = {
        (0, 0): [lambda: relayout(itg_raw, itg_ref), lambda: lax.fori_loop(0, pairs, local, 0, unroll=2)],
        (last, X3): [lambda: x_step(3)],
        (last, X2): [lambda: x_step(2)],
        (last, X1): [lambda: x_step(1)],
        (last, X0): [lambda: x_step(0), lambda: lax.fori_loop(0, pairs, own_part, 0, unroll=2)],
    }
    for time in range(2 * stages + LAG * last):
        for group in range(groups):
            step = time - LAG * group
            if 0 <= step < 2 * stages:
                for h in (2 * group, 2 * group + 1):
                    advance(h, step)
                for work in after.get((group, step), []):
                    work()

    def finish(p, carry):
        total = fetch(cbuf, p, 0).astype(F32) + fetch(cbuf, p, 1).astype(F32) - own[p].astype(F32)
        half_back = dot(turned[p], total.astype(BF)).astype(BF)
        result = loc[p] + dot(half_back, int_ref[p])
        size = (rank_ref[p] + 1) * RSTEP
        result = jnp.where(reach < size, result, 0.0).astype(BF)
        out_ref[p] = jnp.concatenate([result[: R // 2], result[R // 2 :]], axis=1)
        return carry

    lax.fori_loop(0, pairs, finish, 0, unroll=2)

    for h in range(PIECES):
        for s in range(stages):
            reduce_copy(h, s).wait_send()
            gather_copy(1, cbuf, h, s).wait_send()
            gather_copy(2, xbuf, h, s).wait_send()


def tables(orders, list_ref, named_ref, where_ref):
    pairs = list_ref.shape[0]
    stages = len(orders[0])
    units = 1 << stages
    me = jnp.int32(0)
    for axis in AXES:
        me = me * lax.axis_size(axis) + lax.axis_index(axis)

    def clear(i, carry):
        for b in range(8):
            named_ref[i * 8 + b] = pairs
        return carry

    lax.fori_loop(0, units, clear, 0)

    def put(p, carry):
        for e in range(2):
            orbital = list_ref[p, e]
            apart = (orbital >> 1) ^ me
            odd = orbital & 1
            base = (p * 2 + e) * 3
            for o, order in enumerate(orders):
                place = jnp.int32(0)
                for bit in order:
                    place = place * 2 + ((apart >> (bit[2].bit_length() - 1)) & 1)
                where_ref[base + o] = place
                slot = (o * units + place) * 4 + odd * 2
                slot = jnp.where(named_ref[slot] == pairs, slot, slot + 1)
                named_ref[slot] = p
            where_ref[base + 2] = odd
        return carry

    lax.fori_loop(0, pairs, put, 0)


def fused(orders, pair_list, rank_bucket, amplitudes, intersects, integrals, exchange_blocks):
    pairs = amplitudes.shape[0]
    stages = len(orders[0])
    units = 1 << stages
    smem = pl.BlockSpec(memory_space=pltpu.SMEM)
    named, where = pl.pallas_call(
        functools.partial(tables, orders),
        out_shape=(
            jax.ShapeDtypeStruct((2 * units * 4,), jnp.int32),
            jax.ShapeDtypeStruct((pairs * 2 * 3,), jnp.int32),
        ),
        in_specs=[smem],
        out_specs=(smem, smem),
    )(pair_list)

    square = lambda a: a.reshape(a.shape[0], R, R)
    mine = lax.dynamic_slice_in_dim(exchange_blocks, lax.axis_index("gz") * 2, 2, 0)
    rows = R // PIECES
    whole = (PIECES, units, 3, rows, LANES)
    vmem = pl.BlockSpec(memory_space=pltpu.VMEM)
    result = pl.pallas_call(
        functools.partial(kernel, orders),
        out_shape=jax.ShapeDtypeStruct((pairs, R // 2, 2 * R), BF),
        in_specs=[smem] * 3 + [vmem] * 4,
        out_specs=vmem,
        scratch_shapes=[
            pltpu.VMEM((pairs, R, R), BF),
            pltpu.VMEM((pairs, R, R), BF),
            pltpu.VMEM((pairs, R, R), BF),
            pltpu.VMEM((2, R, R), BF),
            pltpu.VMEM((pairs + 1, R, R), BF),
            pltpu.VMEM(whole, BF),
            pltpu.VMEM(whole, BF),
            pltpu.VMEM(whole, BF),
            pltpu.VMEM(whole, BF),
            pltpu.VMEM((pairs, R, R), BF),
            pltpu.VMEM((pairs, R, R), F32),
            pltpu.VMEM((pairs, R, R), BF),
            pltpu.SemaphoreType.DMA((3, PIECES, stages)),
            pltpu.SemaphoreType.DMA((3, PIECES, stages)),
        ],
        compiler_params=pltpu.CompilerParams(
            collective_id=0, has_side_effects=True, vmem_limit_bytes=60 * 1024 * 1024
        ),
    )(rank_bucket, named, where, amplitudes, intersects, integrals, square(mine))
    return result.reshape(pairs, R * R)


def plain(pair_list, rank_bucket, amplitudes, intersects, integrals, exchange_blocks):
    pair_rows, owned_rows = amplitudes.shape[0], exchange_blocks.shape[0]
    square = lambda a: a.reshape(a.shape[0], R, R)
    amplitudes, intersects, integrals = map(square, (amplitudes, intersects, integrals))
    exchange_blocks = square(exchange_blocks)
    occupied = owned_rows * lax.axis_size("gx") * lax.axis_size("gy")
    reach = jnp.maximum(lax.broadcasted_iota(jnp.int32, (R, R), 0), lax.broadcasted_iota(jnp.int32, (R, R), 1))
    inside = reach[None] < ((rank_bucket + 1) * RSTEP)[:, None, None]
    ein = functools.partial(jnp.einsum, preferred_element_type=F32)
    masked = jnp.where(inside, amplitudes, jnp.zeros_like(amplitudes))
    half_projected = ein("pab,pbc->pac", intersects, masked).astype(BF)
    projected = ein("pab,pcb->pac", half_projected, intersects).astype(BF)
    local_term = ein("pab,pbc->pac", masked, integrals)
    counts = jnp.sum(
        (pair_list[None] == lax.broadcasted_iota(jnp.int32, (occupied, 1, 1), 0)).astype(jnp.int32), axis=2
    ).astype(BF)
    share = jnp.dot(counts, projected.reshape(pair_rows, R * R), preferred_element_type=F32)
    share = lax.psum_scatter(share, ("gx", "gy"), scatter_dimension=0, tiled=True)
    domain = lax.psum(share.reshape(owned_rows, R, R), "gz")
    coupled = ein("oab,obc->oac", domain.astype(BF), exchange_blocks).astype(BF)
    every_coupled = lax.all_gather(coupled, ("gx", "gy"), axis=0, tiled=True)
    every_block = lax.all_gather(exchange_blocks, ("gx", "gy"), axis=0, tiled=True)
    own_term = ein("pab,pebc->peac", projected, every_block[pair_list]).astype(BF)
    answers = (every_coupled[pair_list].astype(F32) - own_term.astype(F32)).astype(BF)
    combined = (answers[:, 0].astype(F32) + answers[:, 1].astype(F32)).astype(BF)
    half_back = ein("pba,pbc->pac", intersects, combined).astype(BF)
    total = integrals.astype(F32) + local_term + ein("pab,pbc->pac", half_back, intersects)
    return jnp.where(inside, total, jnp.zeros_like(total)).astype(BF).reshape(pair_rows, R * R)


def solution(mesh):
    shape = dict(mesh.shape)
    split = P(AXES, None)
    powers = all(shape[a] & (shape[a] - 1) == 0 for a in AXES) and shape["gz"] > 1

    def body(*args):
        if powers and args[5].shape[0] == 2 * shape["gz"]:
            return fused(orders_of(shape), *args)
        return plain(*args)

    return jax.shard_map(
        body, mesh=mesh, in_specs=(split, P(AXES), split, split, split, P(("gx", "gy"), None)),
        out_specs=split, check_vma=False,
    )
```

```python
import functools

import jax
import jax.numpy as jnp
import numpy as np
from jax import lax
from jax.experimental import pallas as pl
from jax.experimental.pallas import tpu as pltpu
from jax.sharding import PartitionSpec as P

RSTEP = 64
R = 192
LANES = 128
PIECES = 4
LAG = 1
X2, X1, X0 = 2, 5, 7
AXES = ("gx", "gy", "gz")
MESH = pl.DeviceIdType.MESH
BF = jnp.bfloat16
F32 = jnp.float32


def bits_of(mesh_shape):
    found, stride = {}, 1
    for axis in reversed(AXES):
        size = mesh_shape[axis]
        found[axis] = [(axis, 1 << b, stride << b) for b in range(size.bit_length() - 1)]
        stride *= size
    return found


def orders_of(mesh_shape):
    b = bits_of(mesh_shape)
    first, rest = b["gz"][:1], b["gz"][1:]
    return (first + rest + b["gx"] + b["gy"], first + b["gx"] + rest + b["gy"])


def dot(a, b, dims=((1,), (0,))):
    return lax.dot_general(a, b, (dims, ((), ())), preferred_element_type=F32)


def kernel(
    orders, rank_ref, named_ref, where_ref, amp_raw, int_raw, itg_raw, xown_raw, out_ref,
    amp_ref, int_ref, itg_ref, xown_ref, proj, acc, land, cbuf, xbuf, own, loc, turned, send_sem, recv_sem,
):
    pairs = amp_raw.shape[0]
    stages = len(orders[0])
    units = 1 << stages
    rows = R // PIECES

    def partner(bit):
        axis, stride, _ = bit
        c = lax.axis_index(axis)
        return {axis: c + stride * (1 - 2 * ((c // stride) % 2))}

    order_of = [h % 2 for h in range(PIECES)]
    bit_of = lambda h, s: orders[order_of[h]][s]
    half = lambda s: units >> (s + 1)

    barrier = pltpu.get_barrier_semaphore()
    for bit in orders[0]:
        pl.semaphore_signal(barrier, inc=1, device_id=partner(bit), device_id_type=MESH)
    pl.semaphore_wait(barrier, stages)

    def remote(kind, src, dst, h, s):
        return pltpu.make_async_remote_copy(
            src_ref=src, dst_ref=dst, send_sem=send_sem.at[kind, h, s], recv_sem=recv_sem.at[kind, h, s],
            device_id=partner(bit_of(h, s)), device_id_type=MESH,
        )

    def reduce_copy(h, s):
        n = half(s)
        return remote(0, acc.at[h, pl.ds(n, n)], land.at[h, pl.ds(n, n)], h, s)

    def gather_copy(kind, buf, h, s):
        n = half(s)
        return remote(kind, buf.at[h, pl.ds(0, n)], buf.at[h, pl.ds(n, n)], h, s)

    def pack(ref, h, j, a, b):
        ref[h, j, 0] = a[:, :LANES]
        ref[h, j, 1] = b[:, :LANES]
        ref[h, j, 2] = jnp.concatenate([a[:, LANES:], b[:, LANES:]], axis=1)

    row = lax.broadcasted_iota(jnp.int32, (R, R), 0)
    col = lax.broadcasted_iota(jnp.int32, (R, R), 1)
    natural = jnp.where(row < R // 2, 2 * row, 2 * row - (R - 1))
    reach = jnp.maximum(natural, col)
    sort = (natural == col).astype(F32).astype(BF)

    unsort = (lax.broadcasted_iota(jnp.int32, (R, R), 0) == jnp.where(col < R // 2, 2 * col, 2 * col - (R - 1))).astype(F32).astype(BF)

    for t in range(2):
        xown_ref[t] = dot(dot(sort, xown_raw[t]).astype(BF), sort, ((1,), (1,))).astype(BF)
    for h in range(PIECES):
        span = pl.ds(h * rows, rows)
        pack(xbuf, h, 0, xown_ref[0, span], xown_ref[1, span])
    for h in range(PIECES):
        gather_copy(2, xbuf, h, stages - 1).start()

    def x_step(s):
        for h in range(PIECES):
            gather_copy(2, xbuf, h, s).wait_recv()
            if s:
                gather_copy(2, xbuf, h, s - 1).start()

    def relayout(raw, ref):
        def some(c, carry):
            at = pl.multiple_of(c * 16 * 2 * R, LANES)
            top = pl.multiple_of(c * 16, 16)
            low = pl.multiple_of(R // 2 + c * 16, 16)
            for g in range(0, pairs, 16):
                value = raw[g : g + 16, pl.ds(at, 16 * 2 * R)].reshape(16, 16, 2 * R)
                ref[pl.ds(g, 16), pl.ds(top, 16), :] = value[:, :, :R]
                ref[pl.ds(g, 16), pl.ds(low, 16), :] = value[:, :, R:]
            return carry

        lax.fori_loop(0, R // 32, some, 0)

    def masked(p):
        size = (rank_ref[p] + 1) * RSTEP
        return jnp.where(reach < size, amp_ref[p].astype(F32), 0.0).astype(BF)

    def project(p, carry):
        side = int_ref[p]
        middle = dot(unsort, masked(p)).astype(BF)
        h1 = dot(side, middle).astype(BF)
        proj[p] = dot(h1, side, ((1,), (1,))).astype(BF)
        return carry

    proj[pairs] = jnp.zeros((R, R), BF)
    relayout(amp_raw, amp_ref)
    relayout(int_raw, int_ref)
    lax.fori_loop(0, pairs // 2, project, 0, unroll=8)
    x_step(stages - 1)
    lax.fori_loop(pairs // 2, pairs, project, 0, unroll=8)
    x_step(3)

    def build(h, j, carry):
        span = pl.ds(h * rows, rows)
        base = (order_of[h] * units + j) * 4
        a = proj[named_ref[base], span] + proj[named_ref[base + 1], span]
        b = proj[named_ref[base + 2], span] + proj[named_ref[base + 3], span]
        pack(acc, h, j, a, b)
        return carry

    for h in range(PIECES):
        lax.fori_loop(units // 2, units, functools.partial(build, h), 0, unroll=8)
        reduce_copy(h, 0).start()
    for h in range(PIECES):
        lax.fori_loop(0, units // 2, functools.partial(build, h), 0, unroll=8)

    def local(p, carry):
        block = itg_ref[p]
        middle = dot(unsort, block).astype(BF)
        loc[p] = dot(masked(p), middle) + block.astype(F32)
        turned[p] = dot(sort, int_ref[p], ((1,), (1,))).astype(BF)
        return carry

    def fetch(buf, p, e):
        base = (p * 2 + e) * 3
        odd = where_ref[base + 2]
        parts = []
        for h in range(PIECES):
            at = where_ref[base + order_of[h]]
            tail = buf[h, at, 2]
            tail = jnp.where(odd == 1, tail[:, LANES // 2 :], tail[:, : LANES // 2])
            parts.append(jnp.concatenate([buf[h, at, odd], tail], axis=1))
        return jnp.concatenate(parts, axis=0)

    def own_part(p, carry):
        both = fetch(xbuf, p, 0) + fetch(xbuf, p, 1)
        own[p] = dot(proj[p], both).astype(BF)
        return carry

    def add(h, n, j, carry):
        acc[h, j] = acc[h, j] + land[h, n + j]
        return carry

    def couple(h):
        tail = acc[h, 0, 2]
        done = []
        for t in range(2):
            block = jnp.concatenate([acc[h, 0, t], tail[:, t * (LANES // 2) : (t + 1) * (LANES // 2)]], axis=1)
            done.append(dot(block, xown_ref[t]).astype(BF))
        pack(cbuf, h, 0, *done)
        gather_copy(1, cbuf, h, stages - 1).start()

    def advance(h, step):
        if step >= stages:
            s = 2 * stages - 1 - step
            gather_copy(1, cbuf, h, s).wait_recv()
            if s:
                gather_copy(1, cbuf, h, s - 1).start()
            return
        n = half(step)
        reduce_copy(h, step).wait_recv()
        lax.fori_loop(n // 2, n, functools.partial(add, h, n), 0, unroll=True if n <= 4 else 4)
        if step + 1 < stages:
            reduce_copy(h, step + 1).start()
        lax.fori_loop(0, n // 2, functools.partial(add, h, n), 0, unroll=True if n <= 4 else 4)
        if step + 1 == stages:
            couple(h)

    groups = PIECES // 2
    last = groups - 1
    after = {
        (0, 0): [lambda: relayout(itg_raw, itg_ref), lambda: lax.fori_loop(0, pairs, local, 0, unroll=4)],

        (last, X2): [lambda: x_step(2)],
        (last, X1): [lambda: x_step(1)],
        (last, X0): [lambda: x_step(0), lambda: lax.fori_loop(0, pairs, own_part, 0, unroll=4)],
    }
    for time in range(2 * stages + LAG * last):
        for group in range(groups):
            step = time - LAG * group
            if 0 <= step < 2 * stages:
                for h in (2 * group, 2 * group + 1):
                    advance(h, step)
                for work in after.get((group, step), []):
                    work()

    def finish(p, carry):
        total = fetch(cbuf, p, 0).astype(F32) + fetch(cbuf, p, 1).astype(F32) - own[p].astype(F32)
        half_back = dot(turned[p], total.astype(BF)).astype(BF)
        result = loc[p] + dot(half_back, int_ref[p])
        size = (rank_ref[p] + 1) * RSTEP
        result = jnp.where(reach < size, result, 0.0).astype(BF)
        out_ref[p] = jnp.concatenate([result[: R // 2], result[R // 2 :]], axis=1)
        return carry

    lax.fori_loop(0, pairs, finish, 0, unroll=8)

    for h in range(PIECES):
        for s in range(stages):
            reduce_copy(h, s).wait_send()
            gather_copy(1, cbuf, h, s).wait_send()
            gather_copy(2, xbuf, h, s).wait_send()


def tables(orders, list_ref, named_ref, where_ref):
    pairs = list_ref.shape[0]
    stages = len(orders[0])
    units = 1 << stages
    me = jnp.int32(0)
    for axis in AXES:
        me = me * lax.axis_size(axis) + lax.axis_index(axis)

    def clear(i, carry):
        for b in range(8):
            named_ref[i * 8 + b] = pairs
        return carry

    lax.fori_loop(0, units, clear, 0)

    def put(p, carry):
        for e in range(2):
            orbital = list_ref[p, e]
            apart = (orbital >> 1) ^ me
            odd = orbital & 1
            base = (p * 2 + e) * 3
            for o, order in enumerate(orders):
                place = jnp.int32(0)
                for bit in order:
                    place = place * 2 + ((apart >> (bit[2].bit_length() - 1)) & 1)
                where_ref[base + o] = place
                slot = (o * units + place) * 4 + odd * 2
                slot = jnp.where(named_ref[slot] == pairs, slot, slot + 1)
                named_ref[slot] = p
            where_ref[base + 2] = odd
        return carry

    lax.fori_loop(0, pairs, put, 0)


def fused(orders, pair_list, rank_bucket, amplitudes, intersects, integrals, exchange_blocks):
    pairs = amplitudes.shape[0]
    stages = len(orders[0])
    units = 1 << stages
    smem = pl.BlockSpec(memory_space=pltpu.SMEM)
    named, where = pl.pallas_call(
        functools.partial(tables, orders),
        out_shape=(
            jax.ShapeDtypeStruct((2 * units * 4,), jnp.int32),
            jax.ShapeDtypeStruct((pairs * 2 * 3,), jnp.int32),
        ),
        in_specs=[smem],
        out_specs=(smem, smem),
    )(pair_list)

    square = lambda a: a.reshape(a.shape[0], R, R)
    mine = lax.dynamic_slice_in_dim(exchange_blocks, lax.axis_index("gz") * 2, 2, 0)
    rows = R // PIECES
    whole = (PIECES, units, 3, rows, LANES)
    vmem = pl.BlockSpec(memory_space=pltpu.VMEM)
    result = pl.pallas_call(
        functools.partial(kernel, orders),
        out_shape=jax.ShapeDtypeStruct((pairs, R // 2, 2 * R), BF),
        in_specs=[smem] * 3 + [vmem] * 4,
        out_specs=vmem,
        scratch_shapes=[
            pltpu.VMEM((pairs, R, R), BF),
            pltpu.VMEM((pairs, R, R), BF),
            pltpu.VMEM((pairs, R, R), BF),
            pltpu.VMEM((2, R, R), BF),
            pltpu.VMEM((pairs + 1, R, R), BF),
            pltpu.VMEM(whole, BF),
            pltpu.VMEM(whole, BF),
            pltpu.VMEM(whole, BF),
            pltpu.VMEM(whole, BF),
            pltpu.VMEM((pairs, R, R), BF),
            pltpu.VMEM((pairs, R, R), F32),
            pltpu.VMEM((pairs, R, R), BF),
            pltpu.SemaphoreType.DMA((3, PIECES, stages)),
            pltpu.SemaphoreType.DMA((3, PIECES, stages)),
        ],
        compiler_params=pltpu.CompilerParams(
            collective_id=0, has_side_effects=True, vmem_limit_bytes=60 * 1024 * 1024
        ),
    )(rank_bucket, named, where, amplitudes, intersects, integrals, square(mine))
    return result.reshape(pairs, R * R)


def plain(pair_list, rank_bucket, amplitudes, intersects, integrals, exchange_blocks):
    pair_rows, owned_rows = amplitudes.shape[0], exchange_blocks.shape[0]
    square = lambda a: a.reshape(a.shape[0], R, R)
    amplitudes, intersects, integrals = map(square, (amplitudes, intersects, integrals))
    exchange_blocks = square(exchange_blocks)
    occupied = owned_rows * lax.axis_size("gx") * lax.axis_size("gy")
    reach = jnp.maximum(lax.broadcasted_iota(jnp.int32, (R, R), 0), lax.broadcasted_iota(jnp.int32, (R, R), 1))
    inside = reach[None] < ((rank_bucket + 1) * RSTEP)[:, None, None]
    ein = functools.partial(jnp.einsum, preferred_element_type=F32)
    masked = jnp.where(inside, amplitudes, jnp.zeros_like(amplitudes))
    half_projected = ein("pab,pbc->pac", intersects, masked).astype(BF)
    projected = ein("pab,pcb->pac", half_projected, intersects).astype(BF)
    local_term = ein("pab,pbc->pac", masked, integrals)
    counts = jnp.sum(
        (pair_list[None] == lax.broadcasted_iota(jnp.int32, (occupied, 1, 1), 0)).astype(jnp.int32), axis=2
    ).astype(BF)
    share = jnp.dot(counts, projected.reshape(pair_rows, R * R), preferred_element_type=F32)
    share = lax.psum_scatter(share, ("gx", "gy"), scatter_dimension=0, tiled=True)
    domain = lax.psum(share.reshape(owned_rows, R, R), "gz")
    coupled = ein("oab,obc->oac", domain.astype(BF), exchange_blocks).astype(BF)
    every_coupled = lax.all_gather(coupled, ("gx", "gy"), axis=0, tiled=True)
    every_block = lax.all_gather(exchange_blocks, ("gx", "gy"), axis=0, tiled=True)
    own_term = ein("pab,pebc->peac", projected, every_block[pair_list]).astype(BF)
    answers = (every_coupled[pair_list].astype(F32) - own_term.astype(F32)).astype(BF)
    combined = (answers[:, 0].astype(F32) + answers[:, 1].astype(F32)).astype(BF)
    half_back = ein("pba,pbc->pac", intersects, combined).astype(BF)
    total = integrals.astype(F32) + local_term + ein("pab,pbc->pac", half_back, intersects)
    return jnp.where(inside, total, jnp.zeros_like(total)).astype(BF).reshape(pair_rows, R * R)


def solution(mesh):
    shape = dict(mesh.shape)
    split = P(AXES, None)
    powers = all(shape[a] & (shape[a] - 1) == 0 for a in AXES) and shape["gz"] > 1

    def body(*args):
        if powers and args[5].shape[0] == 2 * shape["gz"]:
            return fused(orders_of(shape), *args)
        return plain(*args)

    return jax.shard_map(
        body, mesh=mesh, in_specs=(split, P(AXES), split, split, split, P(("gx", "gy"), None)),
        out_specs=split, check_vma=False,
    )
```
